32 devices in a mesh: samples: 8 (over z, y), groups: 4 (over x, core).
Axes of the slice: x: 2, y: 2, z: 4, core: 2. Of those that a mesh axis runs over, the one named last changes fastest.
Arguments:
- observed: bfloat16 [128, 10240], P('samples', 'groups'), may hold values from -200 to 200
- labels: int32 [10240], P('groups'), may hold values from 0 to 31, as said below
- comp_sizes: int32 [32], P('groups'), may hold values from 128 to 512, as said below
Outputs:
- whitened: bfloat16 [128, 10240], P('samples', 'groups')
The draws below stay inside these ranges and needn't reach their ends.
Inputs may be any that keep to these rules, and one draw needn't show every extreme that they name: Group g's columns (g * 2560 to (g + 1) * 2560 - 1) carry exactly the labels g * 8 to (g + 1) * 8 - 1, and label c stands on exactly comp_sizes[c] columns. `comp_sizes`: in every group one component has exactly 512 variables; components 2k and 2k + 1 (k = 0, 1, ...) together have exactly 640 variables.
All inputs are finite; a program needn't handle non-finite values. Where the reference program divides by a largest or mean magnitude, that divisor is 1e-20 or more.
Results may differ from the reference program's by a relative error of at most 0.0038.
The reference program's roundings to bfloat16 on the way count: a program that leaves them out, or rounds other values in their place, can miss the bound.
Values may be sent and summed in bfloat16 or wider, within the bound.
A program may use at most 64 MiB of HBM per device.

```python
import math
import jax
import jax.numpy as jnp
from jax import lax

CMAX = 512
ITERS = 5
LOW = 128
AVG = 320
NCG = 8
COMPS = 32
VG = 2560
V = 10240
ROWS = 128


def group_sizes(key):
    base_key = jax.random.fold_in(key, 11)
    spread_key, shuffle_key, flip_key = jax.random.split(base_key, 3)
    group_total = COMPS // NCG
    pair_total = NCG // 2
    offsets = jax.random.randint(spread_key, (group_total, pair_total), 0, AVG - LOW + 1)
    offsets = offsets.at[:, 0].set(CMAX - AVG)
    shuffle_keys = jax.random.split(shuffle_key, group_total)
    offsets = jax.vmap(jax.random.permutation)(shuffle_keys, offsets)
    flips = jax.random.randint(flip_key, (group_total, pair_total), 0, 2) * 2 - 1
    signed = offsets * flips
    paired = jnp.stack([AVG + signed, AVG - signed], axis=2)
    return paired.reshape(group_total, NCG).astype(jnp.int32)


def draw_comp_sizes(key, part):
    return group_sizes(key).reshape(COMPS).astype(jnp.int32)


def draw_labels(key, part):
    group_total = COMPS // NCG
    sizes_table = group_sizes(key)
    ends = jnp.cumsum(sizes_table, axis=1)
    positions = jnp.arange(VG, dtype=jnp.int32)
    local_label = jnp.sum((positions[None, :, None] >= ends[:, None, :]).astype(jnp.int32), axis=2)
    shuffle_keys = jax.random.split(jax.random.fold_in(key, 13), group_total)
    shuffled = jax.vmap(jax.random.permutation)(shuffle_keys, local_label)
    group_offset = jnp.arange(group_total, dtype=jnp.int32)[:, None] * NCG
    return (shuffled + group_offset).reshape(V).astype(jnp.int32)


def draw_observed(key, part):
    base_key = jax.random.fold_in(key, 17)
    noise_key, column_key, row_key = jax.random.split(base_key, 3)
    column_trend = jnp.exp(math.log(3.0) * jnp.arange(V, dtype=jnp.float32) / V)
    row_trend = jnp.exp(math.log(3.0) * jnp.arange(ROWS, dtype=jnp.float32) / ROWS)
    noise = jnp.clip(jax.random.normal(noise_key, (ROWS, V), jnp.float32), -5.0, 5.0)
    column_rough = jnp.exp(jax.random.uniform(column_key, (V,), jnp.float32, 0.0, math.log(2.0)))
    row_rough = jnp.exp(jax.random.uniform(row_key, (ROWS,), jnp.float32, 0.0, math.log(2.0)))
    values = noise * (row_trend * row_rough)[:, None] * (column_trend * column_rough)[None, :]
    return values.astype(jnp.bfloat16)


def setup_inputs(seed: int = 0) -> dict:
    keys = jax.random.split(jax.random.key(seed), 4)
    observed = draw_observed(jax.random.fold_in(keys[3], 71), 0)
    labels = draw_labels(jax.random.fold_in(keys[3], 71), 0)
    comp_sizes = draw_comp_sizes(jax.random.fold_in(keys[3], 71), 0)
    return {"observed": observed, "labels": labels, "comp_sizes": comp_sizes}


shrink = 0.2
ridge = 0.5


def newton_inverse(matrix):
    identity = jnp.eye(matrix.shape[0], dtype=jnp.float32)
    row_bound = jnp.max(jnp.sum(jnp.abs(matrix), axis=1))
    current = identity / row_bound
    for sweep_index in range(ITERS):
        product = jnp.dot(matrix, current, precision=lax.Precision.HIGHEST)
        current = jnp.dot(current, 2.0 * identity - product, precision=lax.Precision.HIGHEST)
    return current


def reference(observed, labels, comp_sizes):
    row_count, var_count = observed.shape
    wide = observed.astype(jnp.float32)
    energy = jnp.sum(jnp.square(wide))
    average = energy / (row_count * var_count)

    def handle(result, component):
        columns = jnp.nonzero(labels == component, size=CMAX, fill_value=var_count)[0].astype(jnp.int32)
        live = (columns < var_count).astype(jnp.float32)
        safe = jnp.minimum(columns, var_count - 1).astype(jnp.int32)
        slot_block = jnp.take(wide, safe, axis=1) * live[None, :]
        covariance = jnp.dot(slot_block.T, slot_block, precision=lax.Precision.HIGHEST) / row_count
        target = jnp.trace(covariance) / comp_sizes[component].astype(jnp.float32)
        diag_lift = shrink * target + ridge * average
        matrix = (1.0 - shrink) * covariance + diag_lift * jnp.eye(CMAX, dtype=jnp.float32)
        inverse = newton_inverse(matrix).astype(jnp.bfloat16).astype(jnp.float32)
        mapped = jnp.dot(slot_block, inverse, precision=lax.Precision.HIGHEST)
        return result.at[:, columns].set(mapped, mode="drop"), None

    initial = jnp.zeros(observed.shape, jnp.float32)
    finished = lax.scan(handle, initial, jnp.arange(COMPS, dtype=jnp.int32))[0]
    return finished.astype(jnp.bfloat16)
```

```python
import functools

import jax
import jax.numpy as jnp
from jax import lax
from jax.experimental import pallas as pl
from jax.experimental.pallas import tpu as pltpu
from jax.sharding import PartitionSpec as P

CMAX = 512
ITERS = 5
LANES = 128
UNROLL_LIMIT = 1024

shrink = 0.2
ridge = 0.5

BF16 = jnp.bfloat16
F32 = jnp.float32
HIGHEST = lax.Precision.HIGHEST
MESH = pl.DeviceIdType.MESH
VMEM = pl.BlockSpec(memory_space=pltpu.VMEM)


def loop(count, step, carry, unrolled):
    if unrolled:
        for i in range(count):
            carry = step(i, carry)
        return carry
    return lax.fori_loop(0, count, step, carry)


def lane_gather(values, index):
    return jnp.take_along_axis(values, index, axis=1)


def pack_kernel(
    slots, label_ref, observed_ref, packed_ref, place_ref, energy_ref, sorted_ref, low_ref, high_ref, turn_ref
):
    tiles, rows, _ = sorted_ref.shape
    first = lax.axis_index("groups") * slots
    slot = lax.broadcasted_iota(jnp.int32, (slots, LANES), 0)
    down = lax.broadcasted_iota(jnp.int32, (LANES, LANES), 0)
    across = lax.broadcasted_iota(jnp.int32, (LANES, LANES), 1)
    upto = (down <= across).astype(BF16)
    ones = jnp.ones((LANES, LANES), BF16)

    def sort_tile(t, carry):
        base, energy = carry
        label = label_ref[pl.ds(t, 1), :] - first
        equal = (label == slot).astype(F32)
        less = (label < slot).astype(F32)
        rank = jnp.dot(equal.astype(BF16), upto, preferred_element_type=F32) - 1.0
        count = jnp.dot(equal.astype(BF16), ones, preferred_element_type=F32)
        before = jnp.dot(less.astype(BF16), ones, preferred_element_type=F32)
        local = jnp.sum(equal * (before + rank), axis=0, keepdims=True).astype(jnp.int32)
        whole = slot.astype(F32) * CMAX + base + rank
        place_ref[pl.ds(t, 1), :] = jnp.sum(equal * whole, axis=0, keepdims=True).astype(jnp.int32)
        block = observed_ref[t]
        choose = (down == local).astype(BF16)
        sorted_ref[t] = lax.dot_general(
            block, choose, (((1,), (1,)), ((), ())), preferred_element_type=F32
        )
        low_ref[t] = base.astype(jnp.int32)
        high_ref[t] = (base + count).astype(jnp.int32)
        turn_ref[t] = (before - base).astype(jnp.int32)
        wide = block.astype(F32)
        square = wide * wide
        for r in range(0, rows, 8):
            energy = energy + square[r : r + 8]
        return base + count, energy

    start = (jnp.zeros((slots, LANES), F32), jnp.zeros((8, LANES), F32))
    unrolled = tiles * slots <= UNROLL_LIMIT
    _, energy = loop(tiles, sort_tile, start, unrolled)
    energy_ref[...] = energy

    lane = lax.broadcasted_iota(jnp.int32, (rows, LANES), 1)
    parts = CMAX // LANES

    def pack_slot(c, carry):
        def add_tile(t, packed):
            low = jnp.broadcast_to(low_ref[t, pl.ds(c, 1), :], (rows, LANES))
            high = jnp.broadcast_to(high_ref[t, pl.ds(c, 1), :], (rows, LANES))
            turn = jnp.broadcast_to(turn_ref[t, pl.ds(c, 1), :], (rows, LANES))
            moved = lane_gather(sorted_ref[t], (lane + turn) & (LANES - 1))
            return tuple(
                jnp.where((lane + q * LANES >= low) & (lane + q * LANES < high), moved, packed[q])
                for q in range(parts)
            )

        zero = jnp.zeros((rows, LANES), F32)
        packed = loop(tiles, add_tile, (zero,) * parts, unrolled)
        for q in range(parts):
            packed_ref[c, :, q * LANES : (q + 1) * LANES] = packed[q].astype(BF16)
        return carry

    loop(slots, pack_slot, 0, unrolled)


def unpack_kernel(place_ref, packed_ref, result_ref, wide_ref):
    tiles, rows, _ = result_ref.shape
    slots = packed_ref.shape[0]
    parts = CMAX // LANES
    unrolled = tiles * slots <= UNROLL_LIMIT

    def widen(c, carry):
        for q in range(parts):
            wide_ref[c * parts + q] = packed_ref[c, :, q * LANES : (q + 1) * LANES].astype(F32)
        return carry

    loop(slots, widen, 0, unrolled)

    def fill_tile(t, carry):
        place = jnp.broadcast_to(place_ref[pl.ds(t, 1), :], (rows, LANES))
        index = place & (LANES - 1)
        tile = place // LANES

        def take(k, value):
            return jnp.where(tile == k, lane_gather(wide_ref[k], index), value)

        value = loop(slots * parts, take, jnp.zeros((rows, LANES), F32), unrolled)
        result_ref[t] = value.astype(BF16)
        return carry

    loop(tiles, fill_tile, 0, unrolled)


def thirds(value):
    high = value.astype(BF16)
    rest = value - high.astype(F32)
    middle = rest.astype(BF16)
    low = (rest - middle.astype(F32)).astype(BF16)
    return high, middle, low


def eye(extent, value):
    down = lax.broadcasted_iota(jnp.int32, (extent, extent), 0)
    across = lax.broadcasted_iota(jnp.int32, (extent, extent), 1)
    return jnp.where(down == across, jnp.broadcast_to(value, (extent, extent)), 0.0)


def scale_and_bound(samples, gram_peak, squares, size, average):
    target = squares / samples / size
    lift = shrink * target + ridge * average
    weight = (1.0 - shrink) / samples
    return weight, lift, weight * gram_peak + lift


def whiten_rows(block, turned, inner, squares, peak, size, average, out):
    samples = block.shape[0]
    weight, lift, bound = scale_and_bound(samples, peak, squares, size, average)
    inverse_bound = 1.0 / bound
    v = inner * (weight * inverse_bound)
    e = 1.0 - lift * inverse_bound
    c = jnp.ones_like(e)
    u = d = None
    for step in range(ITERS):
        last = step == ITERS - 1
        if step == 0:
            new_d = eye(samples, -c)
            new_u = eye(samples, 2.0 * e) - v
        elif step == 1:
            new_d = v - c * u - eye(samples, 1.0 + e)
        else:
            new_d = (1.0 + e) * d - c * u - jnp.dot(d, v, precision=HIGHEST, preferred_element_type=F32)
        if not last:
            if step > 0:
                new_u = 2.0 * e * u - jnp.dot(u, v, precision=HIGHEST, preferred_element_type=F32)
            v = 2.0 * e * v - jnp.dot(v, v, precision=HIGHEST, preferred_element_type=F32)
            u = new_u
        d = new_d
        c = c * (1.0 + e)
        e = e * e
    mixed = sum(jnp.dot(piece, block, preferred_element_type=F32) for piece in reversed(thirds(d)))
    mixed = mixed * (weight * inverse_bound)
    width = block.shape[1]
    stacked = jnp.concatenate(thirds(mixed), axis=0)
    wide_turned = jnp.concatenate([turned] * 3, axis=1)
    inverse = jnp.dot(wide_turned, stacked, preferred_element_type=F32) * inverse_bound
    inverse = (inverse + eye(width, c * inverse_bound)).astype(BF16)
    out(jnp.dot(block, inverse, preferred_element_type=F32).astype(BF16))


def whiten_columns(block, gram_ref, current_ref, squares, peak, size, average, out):
    samples, width = block.shape
    weight, lift, bound = scale_and_bound(samples, peak, squares, size, average)
    gram_ref[...] = weight * gram_ref[...] + eye(width, lift)
    current_ref[...] = eye(width, 1.0 / bound)

    def sweep(i, carry):
        current = current_ref[...]
        product = jnp.dot(gram_ref[...], current, precision=HIGHEST, preferred_element_type=F32)
        current_ref[...] = jnp.dot(
            current, eye(width, jnp.full((1, 1), 2.0, F32)) - product, precision=HIGHEST, preferred_element_type=F32
        )
        return carry

    lax.fori_loop(0, ITERS, sweep, 0)
    out(jnp.dot(block, current_ref[...].astype(BF16), preferred_element_type=F32).astype(BF16))


def exchange_kernel(
    samples_count,
    groups_count,
    entries,
    size_ref,
    packed_ref,
    energy_ref,
    back_ref,
    held_ref,
    done_ref,
    group_ref,
    total_ref,
    all_ref,
    *rest,
):
    *work, group_send, group_recv, total_send, total_recv, out_send, out_recv, back_send, back_recv = rest
    me = lax.axis_index("samples")
    group = lax.axis_index("groups")
    _, slot_here, rows, width = packed_ref.shape
    samples = samples_count * rows

    def ahead(k):
        return lax.rem(me + k, samples_count)

    def behind(k):
        return lax.rem(me + samples_count - k, samples_count)

    def copy(source, target, send, recv, sample, other):
        return pltpu.make_async_remote_copy(
            src_ref=source,
            dst_ref=target,
            send_sem=send,
            recv_sem=recv,
            device_id=(sample, other),
            device_id_type=MESH,
        )

    barrier = pltpu.get_barrier_semaphore()
    for k in range(1, samples_count):
        pl.semaphore_signal(barrier, inc=1, device_id=(ahead(k), group), device_id_type=MESH)
    for k in range(1, groups_count):
        other = lax.rem(group + k, groups_count)
        pl.semaphore_signal(barrier, inc=1, device_id=(me, other), device_id_type=MESH)
    held_ref[0] = packed_ref[me]
    pl.semaphore_wait(barrier, samples_count + groups_count - 2)

    group_copies = [
        copy(
            energy_ref,
            group_ref.at[k - 1],
            group_send.at[k - 1],
            group_recv.at[k - 1],
            me,
            lax.rem(group + k, groups_count),
        )
        for k in range(1, groups_count)
    ]
    out_copies = [
        copy(packed_ref.at[ahead(k)], held_ref.at[k], out_send.at[k - 1], out_recv.at[k - 1], ahead(k), group)
        for k in range(1, samples_count)
    ]
    total_copies = [
        copy(total_ref, all_ref.at[k - 1], total_send.at[k - 1], total_recv.at[k - 1], ahead(k), group)
        for k in range(1, samples_count)
    ]
    back_copies = [
        copy(done_ref.at[k], back_ref.at[me], back_send.at[k - 1], back_recv.at[me], behind(k), group)
        for k in range(1, samples_count)
    ]
    for item in group_copies + out_copies:
        item.start()
    for item in group_copies:
        item.wait_recv()
    total = energy_ref[...]
    for k in range(groups_count - 1):
        total = total + group_ref[k]
    total_ref[...] = total
    for item in total_copies:
        item.start()
    for item in out_copies:
        item.wait_recv()

    average = None
    for h in range(slot_here):
        block = held_ref[:, h].reshape(samples, width)
        turned = block.T
        wide = block.astype(F32)
        squares = jnp.sum(jnp.sum(wide * wide, axis=0, keepdims=True), axis=1, keepdims=True)
        sums = jnp.zeros((1, width), F32)
        for r in range(0, width, LANES):
            part = jnp.dot(turned[r : r + LANES], block, preferred_element_type=F32)
            if work:
                work[0][r : r + LANES, :] = part
            sums = sums + jnp.sum(jnp.abs(part), axis=0, keepdims=True)
        peak = jnp.max(sums, axis=1, keepdims=True)
        if not work:
            inner = lax.dot_general(block, block, (((1,), (1,)), ((), ())), preferred_element_type=F32)
        if average is None:
            for item in total_copies:
                item.wait_recv()
            for k in range(samples_count - 1):
                total = total + all_ref[k]
            energy = jnp.sum(jnp.sum(total, axis=0, keepdims=True), axis=1, keepdims=True)
            average = energy / entries
        size = jnp.full((1, 1), size_ref[me * slot_here + h], jnp.int32).astype(F32)

        def out(value):
            done_ref[:, h] = value.reshape(samples_count, rows, width)

        if work:
            whiten_columns(block, work[0], work[1], squares, peak, size, average, out)
        else:
            whiten_rows(block, turned, inner, squares, peak, size, average, out)

    for item in back_copies:
        item.start()
    back_ref[me] = done_ref[0]
    for k in range(1, samples_count):
        copy(
            done_ref.at[k], back_ref.at[ahead(k)], back_send.at[k - 1], back_recv.at[ahead(k)], ahead(k), group
        ).wait_recv()
    for item in group_copies + out_copies + total_copies + back_copies:
        item.wait_send()


def body(observed, labels, comp_sizes):
    rows, width = observed.shape
    slots = comp_sizes.shape[0]
    samples_count = lax.axis_size("samples")
    groups_count = lax.axis_size("groups")
    slot_here = slots // samples_count
    tiles = width // LANES
    samples = rows * samples_count
    tiled = observed.reshape(rows, tiles, LANES).transpose(1, 0, 2)
    packed, place, energy = pl.pallas_call(
        functools.partial(pack_kernel, slots),
        out_shape=(
            jax.ShapeDtypeStruct((slots, rows, CMAX), BF16),
            jax.ShapeDtypeStruct((tiles, LANES), jnp.int32),
            jax.ShapeDtypeStruct((8, LANES), F32),
        ),
        in_specs=[VMEM] * 2,
        out_specs=(VMEM,) * 3,
        scratch_shapes=[pltpu.VMEM((tiles, rows, LANES), F32)]
        + [pltpu.VMEM((tiles, slots, LANES), jnp.int32)] * 3,
        compiler_params=pltpu.CompilerParams(vmem_limit_bytes=56 * 2**20),
        name="pack",
    )(labels.reshape(tiles, LANES), tiled)

    kind = pltpu.SemaphoreType.DMA
    work = [pltpu.VMEM((CMAX, CMAX), F32)] * 2 if samples >= CMAX else []
    back = pl.pallas_call(
        functools.partial(
            exchange_kernel, samples_count, groups_count, float(samples * width * groups_count)
        ),
        out_shape=jax.ShapeDtypeStruct((samples_count, slot_here, rows, CMAX), BF16),
        in_specs=[pl.BlockSpec(memory_space=pltpu.SMEM), VMEM, VMEM],
        out_specs=VMEM,
        scratch_shapes=[
            pltpu.VMEM((samples_count, slot_here, rows, CMAX), BF16),
            pltpu.VMEM((samples_count, slot_here, rows, CMAX), BF16),
            pltpu.VMEM((groups_count - 1, 8, LANES), F32),
            pltpu.VMEM((8, LANES), F32),
            pltpu.VMEM((samples_count - 1, 8, LANES), F32),
            *work,
            kind((groups_count - 1,)),
            kind((groups_count - 1,)),
            kind((samples_count - 1,)),
            kind((samples_count - 1,)),
            kind((samples_count - 1,)),
            kind((samples_count - 1,)),
            kind((samples_count - 1,)),
            kind((samples_count,)),
        ],
        compiler_params=pltpu.CompilerParams(
            collective_id=0, has_side_effects=True, vmem_limit_bytes=56 * 2**20
        ),
        name="exchange",
    )(comp_sizes, packed.reshape(samples_count, slot_here, rows, CMAX), energy)

    result = pl.pallas_call(
        unpack_kernel,
        out_shape=jax.ShapeDtypeStruct((tiles, rows, LANES), BF16),
        in_specs=[VMEM] * 2,
        out_specs=VMEM,
        scratch_shapes=[pltpu.VMEM((slots * CMAX // LANES, rows, LANES), F32)],
        compiler_params=pltpu.CompilerParams(vmem_limit_bytes=56 * 2**20),
        name="unpack",
    )(place, back.reshape(slots, rows, CMAX))
    return result.transpose(1, 0, 2).reshape(rows, width)


def solution(mesh):
    return jax.shard_map(
        body,
        mesh=mesh,
        in_specs=(P("samples", "groups"), P("groups"), P("groups")),
        out_specs=P("samples", "groups"),
        check_vma=False,
    )
```

```python
import functools

import jax
import jax.numpy as jnp
from jax import lax
from jax.experimental import pallas as pl
from jax.experimental.pallas import tpu as pltpu
from jax.sharding import PartitionSpec as P

CMAX = 512
ITERS = 5
LANES = 128
UNROLL_LIMIT = 1024

shrink = 0.2
ridge = 0.5

BF16 = jnp.bfloat16
F32 = jnp.float32
HIGHEST = lax.Precision.HIGHEST
MESH = pl.DeviceIdType.MESH
VMEM = pl.BlockSpec(memory_space=pltpu.VMEM)


def loop(count, step, carry, unrolled):
    if unrolled:
        for i in range(count):
            carry = step(i, carry)
        return carry
    return lax.fori_loop(0, count, step, carry)


def lane_gather(values, index):
    return jnp.take_along_axis(values, index, axis=1)


def thirds(value):
    high = value.astype(BF16)
    rest = value - high.astype(F32)
    middle = rest.astype(BF16)
    low = (rest - middle.astype(F32)).astype(BF16)
    return high, middle, low


def eye(extent, value):
    down = lax.broadcasted_iota(jnp.int32, (extent, extent), 0)
    across = lax.broadcasted_iota(jnp.int32, (extent, extent), 1)
    return jnp.where(down == across, jnp.broadcast_to(value, (extent, extent)), 0.0)


def scale_and_bound(samples, gram_peak, squares, size, average):
    target = squares / samples / size
    lift = shrink * target + ridge * average
    weight = (1.0 - shrink) / samples
    return weight, lift, weight * gram_peak + lift


def whiten_rows(block, turned, inner, squares, peak, size, average, out):
    samples = block.shape[0]
    weight, lift, bound = scale_and_bound(samples, peak, squares, size, average)
    inverse_bound = 1.0 / bound
    v = inner * (weight * inverse_bound)
    e = 1.0 - lift * inverse_bound
    c = jnp.ones_like(e)
    u = d = None
    for step in range(ITERS):
        last = step == ITERS - 1
        if step == 0:
            new_d = eye(samples, -c)
            new_u = eye(samples, 2.0 * e) - v
        elif step == 1:
            new_d = v - c * u - eye(samples, 1.0 + e)
        else:
            new_d = (1.0 + e) * d - c * u - jnp.dot(d, v, precision=HIGHEST, preferred_element_type=F32)
        if not last:
            if step > 0:
                new_u = 2.0 * e * u - jnp.dot(u, v, precision=HIGHEST, preferred_element_type=F32)
            v = 2.0 * e * v - jnp.dot(v, v, precision=HIGHEST, preferred_element_type=F32)
            u = new_u
        d = new_d
        c = c * (1.0 + e)
        e = e * e
    mixed = sum(jnp.dot(piece, block, preferred_element_type=F32) for piece in reversed(thirds(d)))
    mixed = mixed * (weight * inverse_bound)
    width = block.shape[1]
    stacked = jnp.concatenate(thirds(mixed), axis=0)
    wide_turned = jnp.concatenate([turned] * 3, axis=1)
    inverse = jnp.dot(wide_turned, stacked, preferred_element_type=F32) * inverse_bound
    inverse = (inverse + eye(width, c * inverse_bound)).astype(BF16)
    out(jnp.dot(block, inverse, preferred_element_type=F32).astype(BF16))


def whiten_columns(block, gram_ref, current_ref, squares, peak, size, average, out):
    samples, width = block.shape
    weight, lift, bound = scale_and_bound(samples, peak, squares, size, average)
    gram_ref[...] = weight * gram_ref[...] + eye(width, lift)
    current_ref[...] = eye(width, 1.0 / bound)

    def sweep(i, carry):
        current = current_ref[...]
        product = jnp.dot(gram_ref[...], current, precision=HIGHEST, preferred_element_type=F32)
        current_ref[...] = jnp.dot(
            current, eye(width, jnp.full((1, 1), 2.0, F32)) - product, precision=HIGHEST, preferred_element_type=F32
        )
        return carry

    lax.fori_loop(0, ITERS, sweep, 0)
    out(jnp.dot(block, current_ref[...].astype(BF16), preferred_element_type=F32).astype(BF16))


def fused_kernel(
    samples_count,
    groups_count,
    entries,
    size_ref,
    label_ref,
    observed_ref,
    result_ref,
    sorted_ref,
    low_ref,
    high_ref,
    turn_ref,
    place_ref,
    filled_ref,
    packed_ref,
    held_ref,
    done_ref,
    back_ref,
    energy_ref,
    group_ref,
    total_ref,
    all_ref,
    *rest,
):
    *work, group_send, group_recv, total_send, total_recv, out_send, out_recv, back_send, back_recv = rest
    me = lax.axis_index("samples")
    group = lax.axis_index("groups")
    _, slot_here, rows, width = packed_ref.shape
    samples = samples_count * rows
    slots = samples_count * slot_here
    tiles = sorted_ref.shape[0]
    parts = width // LANES
    unrolled = tiles * slots <= UNROLL_LIMIT
    order = sorted(range(1, samples_count), key=lambda k: abs(2 * k - samples_count))

    def ahead(k):
        return lax.rem(me + k, samples_count)

    def behind(k):
        return lax.rem(me + samples_count - k, samples_count)

    def copy(source, target, send, recv, sample, other):
        return pltpu.make_async_remote_copy(
            src_ref=source,
            dst_ref=target,
            send_sem=send,
            recv_sem=recv,
            device_id=(sample, other),
            device_id_type=MESH,
        )

    def columns(t):
        return pl.ds(t * LANES if isinstance(t, int) else pl.multiple_of(t * LANES, LANES), LANES)

    barrier = pltpu.get_barrier_semaphore()
    for k in range(1, samples_count):
        pl.semaphore_signal(barrier, inc=1, device_id=(ahead(k), group), device_id_type=MESH)
    for k in range(1, groups_count):
        other = lax.rem(group + k, groups_count)
        pl.semaphore_signal(barrier, inc=1, device_id=(me, other), device_id_type=MESH)

    first = group * slots
    slot = lax.broadcasted_iota(jnp.int32, (slots, LANES), 0)
    down = lax.broadcasted_iota(jnp.int32, (LANES, LANES), 0)
    across = lax.broadcasted_iota(jnp.int32, (LANES, LANES), 1)
    upto = (down <= across).astype(BF16)
    ones = jnp.ones((LANES, LANES), BF16)

    def sort_tile(t, carry):
        base, energy = carry
        label = label_ref[pl.ds(t, 1), :] - first
        equal = (label == slot).astype(F32)
        less = (label < slot).astype(F32)
        rank = jnp.dot(equal.astype(BF16), upto, preferred_element_type=F32) - 1.0
        count = jnp.dot(equal.astype(BF16), ones, preferred_element_type=F32)
        before = jnp.dot(less.astype(BF16), ones, preferred_element_type=F32)
        local = jnp.sum(equal * (before + rank), axis=0, keepdims=True).astype(jnp.int32)
        whole = slot.astype(F32) * CMAX + base + rank
        place_ref[pl.ds(t, 1), :] = jnp.sum(equal * whole, axis=0, keepdims=True).astype(jnp.int32)
        block = observed_ref[:, columns(t)]
        choose = (down == local).astype(BF16)
        sorted_ref[t] = lax.dot_general(
            block, choose, (((1,), (1,)), ((), ())), preferred_element_type=F32
        )
        low_ref[t] = base.astype(jnp.int32)
        high_ref[t] = (base + count).astype(jnp.int32)
        turn_ref[t] = (before - base).astype(jnp.int32)
        wide = block.astype(F32)
        square = wide * wide
        for r in range(0, rows, 8):
            energy = energy + square[r : r + 8]
        return base + count, energy

    start = (jnp.zeros((slots, LANES), F32), jnp.zeros((8, LANES), F32))
    _, total = loop(tiles, sort_tile, start, unrolled)
    energy_ref[...] = total

    lane = lax.broadcasted_iota(jnp.int32, (rows, LANES), 1)

    def pack_slot(sample, h, target):
        c = sample * slot_here + h

        def add_tile(t, packed):
            low = jnp.broadcast_to(low_ref[t, pl.ds(c, 1), :], (rows, LANES))
            high = jnp.broadcast_to(high_ref[t, pl.ds(c, 1), :], (rows, LANES))
            turn = jnp.broadcast_to(turn_ref[t, pl.ds(c, 1), :], (rows, LANES))
            moved = lane_gather(sorted_ref[t], (lane + turn) & (LANES - 1))
            return tuple(
                jnp.where((lane + q * LANES >= low) & (lane + q * LANES < high), moved, packed[q])
                for q in range(parts)
            )

        zero = jnp.zeros((rows, LANES), F32)
        packed = loop(tiles, add_tile, (zero,) * parts, unrolled)
        for q in range(parts):
            target[:, q * LANES : (q + 1) * LANES] = packed[q].astype(BF16)

    group_copies = [
        copy(
            energy_ref,
            group_ref.at[k - 1],
            group_send.at[k - 1],
            group_recv.at[k - 1],
            me,
            lax.rem(group + k, groups_count),
        )
        for k in range(1, groups_count)
    ]
    out_copies = {
        k: copy(packed_ref.at[k], held_ref.at[k], out_send.at[k - 1], out_recv.at[k - 1], ahead(k), group)
        for k in order
    }
    total_copies = [
        copy(total_ref, all_ref.at[k - 1], total_send.at[k - 1], total_recv.at[k - 1], ahead(k), group)
        for k in order
    ]
    back_copies = [
        copy(done_ref.at[k], back_ref.at[me], back_send.at[k - 1], back_recv.at[me], behind(k), group)
        for k in order
    ]

    early, late = order[:2], min(6, samples_count - 1)
    for place, k in enumerate(order):
        for h in range(slot_here):
            pack_slot(ahead(k), h, packed_ref.at[k, h])
        if k == early[-1]:
            pl.semaphore_wait(barrier, samples_count + groups_count - 2)
            for item in group_copies:
                item.start()
            for item in early:
                out_copies[item].start()
        elif place >= len(early):
            out_copies[k].start()
        if place == late - 1:
            for item in group_copies:
                item.wait_recv()
            for item in range(groups_count - 1):
                total = total + group_ref[item]
            total_ref[...] = total
            for item in total_copies:
                item.start()
    for h in range(slot_here):
        pack_slot(me, h, held_ref.at[0, h])
    for k in order:
        out_copies[k].wait_recv()

    average = None
    for h in range(slot_here):
        block = held_ref[:, h].reshape(samples, width)
        turned = block.T
        wide = block.astype(F32)
        squares = jnp.sum(jnp.sum(wide * wide, axis=0, keepdims=True), axis=1, keepdims=True)
        sums = jnp.zeros((1, width), F32)
        for r in range(0, width, LANES):
            part = jnp.dot(turned[r : r + LANES], block, preferred_element_type=F32)
            if work:
                work[0][r : r + LANES, :] = part
            sums = sums + jnp.sum(jnp.abs(part), axis=0, keepdims=True)
        peak = jnp.max(sums, axis=1, keepdims=True)
        if not work:
            inner = lax.dot_general(block, block, (((1,), (1,)), ((), ())), preferred_element_type=F32)
        if average is None:
            for item in total_copies:
                item.wait_recv()
            for k in range(samples_count - 1):
                total = total + all_ref[k]
            energy = jnp.sum(jnp.sum(total, axis=0, keepdims=True), axis=1, keepdims=True)
            average = energy / entries
        size = jnp.full((1, 1), size_ref[me * slot_here + h], jnp.int32).astype(F32)

        def out(value):
            done_ref[:, h] = value.reshape(samples_count, rows, width)

        if work:
            whiten_columns(block, work[0], work[1], squares, peak, size, average, out)
        else:
            whiten_rows(block, turned, inner, squares, peak, size, average, out)

    for item in back_copies:
        item.start()

    def fill(sample, source, opening):
        for h in range(slot_here):
            wide = [source[h, :, q * LANES : (q + 1) * LANES].astype(F32) for q in range(parts)]

            def fill_tile(t, carry):
                place = jnp.broadcast_to(place_ref[pl.ds(t, 1), :], (rows, LANES))
                place = place - (sample * slot_here + h) * CMAX
                index = place & (LANES - 1)
                if opening and h == 0:
                    value = jnp.zeros((rows, LANES), F32)
                else:
                    value = filled_ref[t]
                for q in range(parts):
                    inside = (place >= q * LANES) & (place < (q + 1) * LANES)
                    value = jnp.where(inside, lane_gather(wide[q], index), value)
                filled_ref[t] = value
                return carry

            loop(tiles, fill_tile, 0, unrolled)

    fill(me, done_ref.at[0], True)
    for k in reversed(order):
        copy(
            done_ref.at[k], back_ref.at[ahead(k)], back_send.at[k - 1], back_recv.at[ahead(k)], ahead(k), group
        ).wait_recv()
        fill(ahead(k), back_ref.at[ahead(k)], False)

    def finish(t, carry):
        result_ref[:, columns(t)] = filled_ref[t].astype(BF16)
        return carry

    loop(tiles, finish, 0, unrolled)
    for item in group_copies + list(out_copies.values()) + total_copies + back_copies:
        item.wait_send()


def body(observed, labels, comp_sizes):
    rows, width = observed.shape
    slots = comp_sizes.shape[0]
    samples_count = lax.axis_size("samples")
    groups_count = lax.axis_size("groups")
    slot_here = slots // samples_count
    tiles = width // LANES
    samples = rows * samples_count
    kind = pltpu.SemaphoreType.DMA
    table = pltpu.VMEM((tiles, slots, LANES), jnp.int32)
    wide_tiles = pltpu.VMEM((tiles, rows, LANES), F32)
    blocks = pltpu.VMEM((samples_count, slot_here, rows, CMAX), BF16)
    work = [pltpu.VMEM((CMAX, CMAX), F32)] * 2 if samples >= CMAX else []
    return pl.pallas_call(
        functools.partial(
            fused_kernel, samples_count, groups_count, float(samples * width * groups_count)
        ),
        out_shape=jax.ShapeDtypeStruct((rows, width), BF16),
        in_specs=[pl.BlockSpec(memory_space=pltpu.SMEM), VMEM, VMEM],
        out_specs=VMEM,
        scratch_shapes=[
            wide_tiles,
            table,
            table,
            table,
            pltpu.VMEM((tiles, LANES), jnp.int32),
            wide_tiles,
            blocks,
            blocks,
            blocks,
            blocks,
            pltpu.VMEM((8, LANES), F32),
            pltpu.VMEM((groups_count - 1, 8, LANES), F32),
            pltpu.VMEM((8, LANES), F32),
            pltpu.VMEM((samples_count - 1, 8, LANES), F32),
            *work,
            kind((groups_count - 1,)),
            kind((groups_count - 1,)),
            kind((samples_count - 1,)),
            kind((samples_count - 1,)),
            kind((samples_count - 1,)),
            kind((samples_count - 1,)),
            kind((samples_count - 1,)),
            kind((samples_count,)),
        ],
        compiler_params=pltpu.CompilerParams(
            collective_id=0, has_side_effects=True, vmem_limit_bytes=56 * 2**20
        ),
        name="whiten",
    )(comp_sizes, labels.reshape(tiles, LANES), observed)


def solution(mesh):
    return jax.shard_map(
        body,
        mesh=mesh,
        in_specs=(P("samples", "groups"), P("groups"), P("groups")),
        out_specs=P("samples", "groups"),
        check_vma=False,
    )
```

```python
import functools

import jax
import jax.numpy as jnp
from jax import lax
from jax.experimental import pallas as pl
from jax.experimental.pallas import tpu as pltpu
from jax.sharding import PartitionSpec as P

CMAX = 512
ITERS = 5
LANES = 128
UNROLL_LIMIT = 1024

shrink = 0.2
ridge = 0.5

BF16 = jnp.bfloat16
F32 = jnp.float32
HIGHEST = lax.Precision.HIGHEST
MESH = pl.DeviceIdType.MESH
VMEM = pl.BlockSpec(memory_space=pltpu.VMEM)


def loop(count, step, carry, unrolled):
    if unrolled:
        for i in range(count):
            carry = step(i, carry)
        return carry
    return lax.fori_loop(0, count, step, carry)


def lane_gather(values, index):
    return jnp.take_along_axis(values, index, axis=1)


def thirds(value):
    high = value.astype(BF16)
    rest = value - high.astype(F32)
    middle = rest.astype(BF16)
    low = (rest - middle.astype(F32)).astype(BF16)
    return high, middle, low


def products(lefts, right):
    extent = right.shape[0]
    high, middle, low = thirds(right)
    left_high, left_middle, left_low = thirds(jnp.concatenate(lefts, axis=0))
    pair = jnp.concatenate([high, middle], axis=1)
    main = jnp.dot(
        jnp.concatenate([left_high, left_middle], axis=1),
        jnp.concatenate([pair, pair], axis=0),
        preferred_element_type=F32,
    )
    small = jnp.dot(
        jnp.concatenate([left_high, left_low], axis=1),
        jnp.concatenate([low, high], axis=0),
        preferred_element_type=F32,
    )
    whole = (small + main[:, extent:]) + main[:, :extent]
    return [whole[i * extent : (i + 1) * extent] for i in range(len(lefts))]


def eye(extent, value):
    down = lax.broadcasted_iota(jnp.int32, (extent, extent), 0)
    across = lax.broadcasted_iota(jnp.int32, (extent, extent), 1)
    return jnp.where(down == across, jnp.broadcast_to(value, (extent, extent)), 0.0)


def scale_and_bound(samples, gram_peak, squares, size, average):
    target = squares / samples / size
    lift = shrink * target + ridge * average
    weight = (1.0 - shrink) / samples
    return weight, lift, weight * gram_peak + lift


def whiten_rows(block, turned, inner, squares, peak, size, average, out):
    samples = block.shape[0]
    weight, lift, bound = scale_and_bound(samples, peak, squares, size, average)
    inverse_bound = 1.0 / bound
    v = inner * (weight * inverse_bound)
    e = 1.0 - lift * inverse_bound
    c = jnp.ones_like(e)
    u = d = None
    for step in range(ITERS):
        lefts = [] if step == ITERS - 1 else [v] if step == 0 else [v, u]
        results = products(lefts + ([d] if step > 1 else []), v)
        if step == 0:
            d, u = eye(samples, -c), eye(samples, 2.0 * e) - v
        else:
            through = results[-1] if step > 1 else -v
            d = (1.0 + e) * d - c * u - through
            if lefts:
                u = 2.0 * e * u - results[1]
        if lefts:
            v = 2.0 * e * v - results[0]
        c = c * (1.0 + e)
        e = e * e
    mixed = sum(jnp.dot(piece, block, preferred_element_type=F32) for piece in reversed(thirds(d)))
    mixed = mixed * (weight * inverse_bound)
    width = block.shape[1]
    stacked = jnp.concatenate(thirds(mixed), axis=0)
    wide_turned = jnp.concatenate([turned] * 3, axis=1)
    inverse = jnp.dot(wide_turned, stacked, preferred_element_type=F32) * inverse_bound
    inverse = (inverse + eye(width, c * inverse_bound)).astype(BF16)
    out(jnp.dot(block, inverse, preferred_element_type=F32).astype(BF16))


def whiten_columns(block, gram_ref, current_ref, squares, peak, size, average, out):
    samples, width = block.shape
    weight, lift, bound = scale_and_bound(samples, peak, squares, size, average)
    gram_ref[...] = weight * gram_ref[...] + eye(width, lift)
    current_ref[...] = eye(width, 1.0 / bound)

    def sweep(i, carry):
        current = current_ref[...]
        product = jnp.dot(gram_ref[...], current, precision=HIGHEST, preferred_element_type=F32)
        current_ref[...] = jnp.dot(
            current, eye(width, jnp.full((1, 1), 2.0, F32)) - product, precision=HIGHEST, preferred_element_type=F32
        )
        return carry

    lax.fori_loop(0, ITERS, sweep, 0)
    out(jnp.dot(block, current_ref[...].astype(BF16), preferred_element_type=F32).astype(BF16))


def fused_kernel(
    samples_count,
    groups_count,
    entries,
    size_hbm,
    label_hbm,
    observed_hbm,
    result_ref,
    size_ref,
    label_ref,
    observed_ref,
    load_sem,
    sorted_ref,
    high_ref,
    turn_ref,
    place_ref,
    filled_ref,
    packed_ref,
    held_ref,
    done_ref,
    back_ref,
    energy_ref,
    group_ref,
    total_ref,
    all_ref,
    *rest,
):
    *work, group_send, group_recv, total_send, total_recv, out_send, out_recv, back_send, back_recv = rest
    me = lax.axis_index("samples")
    group = lax.axis_index("groups")
    _, slot_here, rows, width = packed_ref.shape
    samples = samples_count * rows
    slots = samples_count * slot_here
    tiles = sorted_ref.shape[0]
    parts = width // LANES
    unrolled = tiles * slots <= UNROLL_LIMIT
    order = sorted(range(1, samples_count), key=lambda k: abs(2 * k - samples_count))

    def ahead(k):
        return lax.rem(me + k, samples_count)

    def behind(k):
        return lax.rem(me + samples_count - k, samples_count)

    def copy(source, target, send, recv, sample, other):
        return pltpu.make_async_remote_copy(
            src_ref=source,
            dst_ref=target,
            send_sem=send,
            recv_sem=recv,
            device_id=(sample, other),
            device_id_type=MESH,
        )

    def columns(t):
        return pl.ds(t * LANES if isinstance(t, int) else pl.multiple_of(t * LANES, LANES), LANES)

    loads = [
        pltpu.make_async_copy(source, target, load_sem.at[i])
        for i, (source, target) in enumerate(
            ((label_hbm, label_ref), (observed_hbm, observed_ref), (size_hbm, size_ref))
        )
    ]
    for item in loads:
        item.start()
    barrier = pltpu.get_barrier_semaphore()
    for k in range(1, samples_count):
        pl.semaphore_signal(barrier, inc=1, device_id=(ahead(k), group), device_id_type=MESH)
    for k in range(1, groups_count):
        other = lax.rem(group + k, groups_count)
        pl.semaphore_signal(barrier, inc=1, device_id=(me, other), device_id_type=MESH)

    for item in loads:
        item.wait()

    first = group * slots
    slot = lax.broadcasted_iota(jnp.int32, (slots, LANES), 0)
    down = lax.broadcasted_iota(jnp.int32, (LANES, LANES), 0)
    across = lax.broadcasted_iota(jnp.int32, (LANES, LANES), 1)
    upto = (down <= across).astype(BF16)
    ones = jnp.ones((LANES, LANES), BF16)

    def compare(t):
        label = label_ref[pl.ds(t, 1), :] - first
        return (label == slot).astype(F32), (label < slot).astype(F32)

    def counts(equal, less):
        rank = jnp.dot(equal.astype(BF16), upto, preferred_element_type=F32) - 1.0
        count = jnp.dot(equal.astype(BF16), ones, preferred_element_type=F32)
        before = jnp.dot(less.astype(BF16), ones, preferred_element_type=F32)
        return rank, count, before

    if unrolled:
        pairs = [compare(t) for t in range(tiles)]
        stacked = counts(*(jnp.concatenate(items, axis=0) for items in zip(*pairs)))

    def sort_tile(t, carry):
        base, energy = carry
        if unrolled:
            equal = pairs[t][0]
            rank, count, before = (item[t * slots : (t + 1) * slots] for item in stacked)
        else:
            equal, less = compare(t)
            rank, count, before = counts(equal, less)
        local = jnp.sum(equal * (before + rank), axis=0, keepdims=True).astype(jnp.int32)
        whole = slot.astype(F32) * CMAX + base + rank
        place_ref[pl.ds(t, 1), :] = jnp.sum(equal * whole, axis=0, keepdims=True).astype(jnp.int32)
        block = observed_ref[:, columns(t)]
        choose = (down == local).astype(BF16)
        sorted_ref[t] = lax.dot_general(
            block, choose, (((1,), (1,)), ((), ())), preferred_element_type=F32
        )
        high_ref[t] = (base + count).astype(jnp.int32)
        turn_ref[t] = (before - base).astype(jnp.int32)
        wide = block.astype(F32)
        square = wide * wide
        for r in range(0, rows, 8):
            energy = energy + square[r : r + 8]
        return base + count, energy

    start = (jnp.zeros((slots, LANES), F32), jnp.zeros((8, LANES), F32))
    _, total = loop(tiles, sort_tile, start, unrolled)
    energy_ref[...] = total

    lane = lax.broadcasted_iota(jnp.int32, (rows, LANES), 1)

    def pack_slot(sample, h, target):
        c = sample * slot_here + h

        def add_tile(i, packed):
            t = tiles - 1 - i
            high = jnp.broadcast_to(high_ref[t, pl.ds(c, 1), :], (rows, LANES))
            turn = jnp.broadcast_to(turn_ref[t, pl.ds(c, 1), :], (rows, LANES))
            moved = lane_gather(sorted_ref[t], (lane + turn) & (LANES - 1))
            return tuple(
                jnp.where(lane + q * LANES < high, moved, packed[q])
                for q in range(parts)
            )

        zero = jnp.zeros((rows, LANES), F32)
        packed = loop(tiles, add_tile, (zero,) * parts, unrolled)
        for q in range(parts):
            target[:, q * LANES : (q + 1) * LANES] = packed[q].astype(BF16)

    group_copies = [
        copy(
            energy_ref,
            group_ref.at[k - 1],
            group_send.at[k - 1],
            group_recv.at[k - 1],
            me,
            lax.rem(group + k, groups_count),
        )
        for k in range(1, groups_count)
    ]
    out_copies = {
        k: copy(packed_ref.at[k], held_ref.at[k], out_send.at[k - 1], out_recv.at[k - 1], ahead(k), group)
        for k in order
    }
    total_copies = [
        copy(total_ref, all_ref.at[k - 1], total_send.at[k - 1], total_recv.at[k - 1], ahead(k), group)
        for k in order
    ]
    back_copies = [
        copy(done_ref.at[k], back_ref.at[me], back_send.at[k - 1], back_recv.at[me], behind(k), group)
        for k in order
    ]

    for k in order:
        for h in range(slot_here):
            pack_slot(ahead(k), h, packed_ref.at[k, h])
    pl.semaphore_wait(barrier, samples_count + groups_count - 2)
    for item in group_copies:
        item.start()
    for k in order:
        out_copies[k].start()
    for h in range(slot_here):
        pack_slot(me, h, held_ref.at[0, h])
    for item in group_copies:
        item.wait_recv()
    for k in range(groups_count - 1):
        total = total + group_ref[k]
    total_ref[...] = total
    for item in total_copies:
        item.start()
    for k in order:
        out_copies[k].wait_recv()

    average = None
    for h in range(slot_here):
        block = held_ref[:, h].reshape(samples, width)
        turned = block.T
        wide = block.astype(F32)
        squares = jnp.sum(jnp.sum(wide * wide, axis=0, keepdims=True), axis=1, keepdims=True)
        sums = jnp.zeros((1, width), F32)
        for r in range(0, width, LANES):
            part = jnp.dot(turned[r : r + LANES], block, preferred_element_type=F32)
            if work:
                work[0][r : r + LANES, :] = part
            sums = sums + jnp.sum(jnp.abs(part), axis=0, keepdims=True)
        peak = jnp.max(sums, axis=1, keepdims=True)
        if not work:
            inner = lax.dot_general(block, block, (((1,), (1,)), ((), ())), preferred_element_type=F32)
        if average is None:
            for item in total_copies:
                item.wait_recv()
            for k in range(samples_count - 1):
                total = total + all_ref[k]
            energy = jnp.sum(jnp.sum(total, axis=0, keepdims=True), axis=1, keepdims=True)
            average = energy / entries
        size = jnp.full((1, 1), size_ref[me * slot_here + h], jnp.int32).astype(F32)

        def out(value):
            done_ref[:, h] = value.reshape(samples_count, rows, width)

        if work:
            whiten_columns(block, work[0], work[1], squares, peak, size, average, out)
        else:
            whiten_rows(block, turned, inner, squares, peak, size, average, out)

    for item in back_copies:
        item.start()

    def fill(sample, source, opening):
        for h in range(slot_here):
            wide = [source[h, :, q * LANES : (q + 1) * LANES].astype(F32) for q in range(parts)]

            def fill_tile(t, carry):
                place = jnp.broadcast_to(place_ref[pl.ds(t, 1), :], (rows, LANES))
                index = place & (LANES - 1)
                tile = (place >> (LANES.bit_length() - 1)) - (sample * slot_here + h) * parts
                if opening and h == 0:
                    value = jnp.zeros((rows, LANES), F32)
                else:
                    value = filled_ref[t]
                for q in range(parts):
                    value = jnp.where(tile == q, lane_gather(wide[q], index), value)
                filled_ref[t] = value
                return carry

            loop(tiles, fill_tile, 0, unrolled)

    fill(me, done_ref.at[0], True)
    for k in reversed(order):
        copy(
            done_ref.at[k], back_ref.at[ahead(k)], back_send.at[k - 1], back_recv.at[ahead(k)], ahead(k), group
        ).wait_recv()
        fill(ahead(k), back_ref.at[ahead(k)], False)

    def finish(t, carry):
        result_ref[:, columns(t)] = filled_ref[t].astype(BF16)
        return carry

    loop(tiles, finish, 0, unrolled)
    for item in group_copies + list(out_copies.values()) + total_copies + back_copies:
        item.wait_send()


def body(observed, labels, comp_sizes):
    rows, width = observed.shape
    slots = comp_sizes.shape[0]
    samples_count = lax.axis_size("samples")
    groups_count = lax.axis_size("groups")
    slot_here = slots // samples_count
    tiles = width // LANES
    samples = rows * samples_count
    kind = pltpu.SemaphoreType.DMA
    table = pltpu.VMEM((tiles, slots, LANES), jnp.int32)
    wide_tiles = pltpu.VMEM((tiles, rows, LANES), F32)
    blocks = pltpu.VMEM((samples_count, slot_here, rows, CMAX), BF16)
    work = [pltpu.VMEM((CMAX, CMAX), F32)] * 2 if samples >= CMAX else []
    return pl.pallas_call(
        functools.partial(
            fused_kernel, samples_count, groups_count, float(samples * width * groups_count)
        ),
        out_shape=jax.ShapeDtypeStruct((rows, width), BF16),
        in_specs=[pl.BlockSpec(memory_space=pltpu.HBM)] * 3,
        out_specs=VMEM,
        scratch_shapes=[
            pltpu.SMEM(comp_sizes.shape, jnp.int32),
            pltpu.VMEM((tiles, LANES), jnp.int32),
            pltpu.VMEM((rows, width), BF16),
            kind((3,)),
            wide_tiles,
            table,
            table,
            pltpu.VMEM((tiles, LANES), jnp.int32),
            wide_tiles,
            blocks,
            blocks,
            blocks,
            blocks,
            pltpu.VMEM((8, LANES), F32),
            pltpu.VMEM((groups_count - 1, 8, LANES), F32),
            pltpu.VMEM((8, LANES), F32),
            pltpu.VMEM((samples_count - 1, 8, LANES), F32),
            *work,
            kind((groups_count - 1,)),
            kind((groups_count - 1,)),
            kind((samples_count - 1,)),
            kind((samples_count - 1,)),
            kind((samples_count - 1,)),
            kind((samples_count - 1,)),
            kind((samples_count - 1,)),
            kind((samples_count,)),
        ],
        compiler_params=pltpu.CompilerParams(
            collective_id=0, has_side_effects=True, vmem_limit_bytes=56 * 2**20
        ),
        name="whiten",
    )(comp_sizes, labels.reshape(tiles, LANES), observed)


def solution(mesh):
    return jax.shard_map(
        body,
        mesh=mesh,
        in_specs=(P("samples", "groups"), P("groups"), P("groups")),
        out_specs=P("samples", "groups"),
        check_vma=False,
    )
```
